256 devices in a mesh: doc: 16 (over y_lo, z), seq: 16 (over x, y_hi, core).
Axes of the slice: x: 4, y: 4 (y_hi: 2, y_lo: 2; y = y_hi * 2 + y_lo), z: 8, core: 2. Of those that a mesh axis runs over, the one named last changes fastest.
Arguments:
- queries: bfloat16 [131072, 512], P(('doc', 'seq')), parts along dimension 0, may hold values from -5 to 5
- teacher_keys: bfloat16 [131072, 128], P(('doc', 'seq')), parts along dimension 0, may hold values from -5 to 5
- teacher_values: bfloat16 [131072, 128], P(('doc', 'seq')), parts along dimension 0, may hold values from -5 to 5
- beacon_starts: int32 [8192], P(('doc', 'seq')), parts along dimension 0, may hold values from 0 to 511, as said below
Outputs:
- output_gap: bfloat16 [131072, 512], P(('doc', 'seq')), parts along dimension 0
- beacon_key_grad: float32 [8192, 128], P(('doc', 'seq')), parts along dimension 0
- beacon_value_grad: float32 [8192, 128], P(('doc', 'seq')), parts along dimension 0
The draws below stay inside these ranges and needn't reach their ends.
There are 16 independent parts, one for each index of `doc`. The reference program is written for one: setup_inputs(seed, part) draws one part's arguments, and reference() takes and returns one part's arrays. A program takes and returns all parts, laid end to end along the dimension named above; each array names one. Nothing has to cross between parts.
Inputs may be any that keep to these rules, and one draw needn't show every extreme that they name: `beacon_starts`: each aligned block of 32 entries belongs to one shard of 512 tokens: its first entry is 0 and its entries rise strictly.
All inputs are finite; a program needn't handle non-finite values.
Results may differ from the reference program's by a relative error of at most 0.009.
Values may be sent and summed in bfloat16 or wider, within the bound.
No kernel may reach another device: no remote copies, remote signals or barrier semaphores. Data moves between devices by JAX's collectives and lax.ppermute only.
A program may use at most 192 MiB of HBM per device.

```python
import jax
import jax.numpy as jnp
from jax import lax

HEAD = 128
H = 4
TOK_DEV = 512
BEAC = 32
TOKENS = 8192
N_SEQ = 16


def drawn(key):
    seq_tokens = TOK_DEV * N_SEQ
    base_key = jax.random.fold_in(key, 401)
    query_key, keys_key = jax.random.split(base_key, 2)
    queries = jnp.clip(1.41 * jax.random.normal(query_key, (seq_tokens, H * HEAD), jnp.float32), -4.5, 4.5)
    teacher_keys = jnp.clip(1.41 * jax.random.normal(keys_key, (seq_tokens, HEAD), jnp.float32), -4.5, 4.5)
    return (queries, teacher_keys)


def draw_queries(key, part):
    return drawn(key)[0].astype(jnp.bfloat16)


def draw_teacher_keys(key, part):
    return drawn(key)[1].astype(jnp.bfloat16)


def draw_beacon_starts(key, part):
    base_key = jax.random.fold_in(key, 733)

    def shard_starts(shard_key):
        picked = jax.random.permutation(shard_key, TOK_DEV - 1)[:BEAC - 1] + 1
        return jnp.concatenate([jnp.zeros((1,), jnp.int32), jnp.sort(picked).astype(jnp.int32)])
    return jax.vmap(shard_starts)(jax.random.split(base_key, N_SEQ)).reshape(N_SEQ * BEAC)


def block_levels(rng, dims, cuts, least, top_value):
    factor_of, own = 1.0, jax.random.fold_in(rng, 6)
    for axis_at, blocks in cuts:
        draws = jnp.exp(jax.random.uniform(jax.random.fold_in(own, axis_at), (blocks,), jnp.float32, least / len(cuts), top_value / len(cuts)))
        factor_of = factor_of * jnp.repeat(draws, dims[axis_at] // blocks).reshape([-1 if axis == axis_at else 1 for axis in range(len(dims))])
    return factor_of


def gaussian(rng, extent, scale, limit, shards=(), kind=jnp.bfloat16):
    drawn = scale * jax.random.normal(rng, extent, jnp.float32)
    if shards:
        drawn = drawn * block_levels(rng, extent, shards, -0.22, 0.18)
    return jnp.clip(drawn, -limit, limit).astype(kind)


def setup_inputs(seed: int = 0, part: int = 0) -> dict:
    seeds = jax.random.split(jax.random.key(seed), 5)
    part_splits = jax.random.split(jax.random.fold_in(seeds[4], part), 5)
    return {
        "queries": draw_queries(jax.random.fold_in(jax.random.fold_in(seeds[4], part), 71), part),
        "teacher_keys": draw_teacher_keys(jax.random.fold_in(jax.random.fold_in(seeds[4], part), 71), part),
        "teacher_values": gaussian(part_splits[2], (TOKENS, HEAD), 1.0, 5.0, ((0, 16),)),
        "beacon_starts": draw_beacon_starts(jax.random.fold_in(jax.random.fold_in(seeds[4], part), 71), part),
    }


def pooled_beacons(teacher_keys, teacher_values, beacon_starts):
    positions = jnp.arange(TOK_DEV, dtype=jnp.int32)
    firsts = beacon_starts.reshape(N_SEQ, BEAC)
    endings = jnp.concatenate([firsts[:, 1:], jnp.full((N_SEQ, 1), TOK_DEV, jnp.int32)], axis=1)
    member = ((positions[None, None, :] >= firsts[:, :, None]) & (positions[None, None, :] < endings[:, :, None])).astype(jnp.float32)
    counts = jnp.sum(member, axis=2)
    joined = jnp.concatenate([teacher_keys, teacher_values], axis=1).astype(jnp.float32).reshape(N_SEQ, TOK_DEV, 2 * HEAD)
    pooled_sums = jnp.einsum("sbt,std->sbd", member, joined)
    return (pooled_sums / counts[:, :, None]).astype(jnp.bfloat16).reshape(N_SEQ * BEAC, 2 * HEAD)


def reference(queries, teacher_keys, teacher_values, beacon_starts):
    scaling = HEAD ** -0.5
    beacons = pooled_beacons(teacher_keys, teacher_values, beacon_starts)
    beacon_count = N_SEQ * BEAC
    owners = jnp.arange(beacon_count, dtype=jnp.int32) // BEAC
    seq_tokens = TOK_DEV * N_SEQ
    row_count = TOK_DEV * H
    local_pos = jnp.arange(row_count, dtype=jnp.int32) // H
    key_index = jnp.arange(seq_tokens, dtype=jnp.int32)
    positions = jnp.arange(TOK_DEV, dtype=jnp.int32)

    def shard_step(carried, shard_index):
        first_token = shard_index * TOK_DEV
        query_rows = lax.dynamic_slice_in_dim(queries, first_token, TOK_DEV, 0).reshape(row_count, HEAD)
        scores = jnp.dot(query_rows, teacher_keys.T, preferred_element_type=jnp.float32) * scaling
        scores = jnp.where(key_index[None, :] <= (first_token + local_pos)[:, None], scores, -jnp.inf)
        weights = jnp.exp(scores - jnp.max(scores, axis=1, keepdims=True))
        teacher = jnp.dot(weights.astype(jnp.bfloat16), teacher_values, preferred_element_type=jnp.float32) / jnp.sum(weights, axis=1, keepdims=True)
        local_keys = lax.dynamic_slice_in_dim(teacher_keys, first_token, TOK_DEV, 0)
        local_values = lax.dynamic_slice_in_dim(teacher_values, first_token, TOK_DEV, 0)
        keys_all = jnp.concatenate([beacons[:, :HEAD], local_keys], axis=0)
        values_all = jnp.concatenate([beacons[:, HEAD:], local_values], axis=0)
        visible = jnp.concatenate([jnp.broadcast_to(owners[None, :] < shard_index, (row_count, beacon_count)), positions[None, :] <= local_pos[:, None]], axis=1)
        student_scores = jnp.where(visible, jnp.dot(query_rows, keys_all.T, preferred_element_type=jnp.float32) * scaling, -jnp.inf)
        student_weights = jnp.exp(student_scores - jnp.max(student_scores, axis=1, keepdims=True))
        student_probs = student_weights / jnp.sum(student_weights, axis=1, keepdims=True)
        probs_low = student_probs.astype(jnp.bfloat16)
        student = jnp.dot(probs_low, values_all, preferred_element_type=jnp.float32)
        output_gap = (student - teacher).astype(jnp.bfloat16)
        prob_grad = jnp.dot(output_gap, values_all.T, preferred_element_type=jnp.float32)
        row_dot = jnp.sum(student_probs * prob_grad, axis=1, keepdims=True)
        score_grad = (student_probs * (prob_grad - row_dot)).astype(jnp.bfloat16)
        grad_keys = jnp.dot(score_grad[:, :beacon_count].T, query_rows, preferred_element_type=jnp.float32) * scaling
        grad_values = jnp.dot(probs_low[:, :beacon_count].T, output_gap, preferred_element_type=jnp.float32)
        return carried + jnp.concatenate([grad_keys, grad_values], axis=1), output_gap.reshape(TOK_DEV, H * HEAD)

    initial = jnp.zeros((beacon_count, 2 * HEAD), jnp.float32)
    grads, gaps = lax.scan(shard_step, initial, jnp.arange(N_SEQ, dtype=jnp.int32))
    return (gaps.reshape(seq_tokens, H * HEAD), grads[:, :HEAD], grads[:, HEAD:])
```

```python
import functools

import jax
import jax.numpy as jnp
from jax import lax
from jax.experimental import pallas as pl
from jax.experimental.pallas import tpu as pltpu
from jax.sharding import PartitionSpec as P


HEADS = 4
HEAD = 128
TOK = 512
BEAC = 32
SEQ = 16
ROWS = TOK + BEAC
SCALE = HEAD**-0.5
LOG2E = 1.4426950408889634
C2 = SCALE * LOG2E
F32 = jnp.float32
BF16 = jnp.bfloat16


def dot(a, b):
    return jnp.dot(a, b, preferred_element_type=F32)


def split_index(s):
    return s // 4, (s // 2) % 2, s % 2


def placed(s, dx, dy, dc):
    x, y, c = split_index(s)
    return ((x + dx) % 4) * 4 + (y + dy) % 2 * 2 + (c + dc) % 2


def whole(*shape):
    return pl.BlockSpec(shape, lambda: tuple(0 for _ in shape))


def prep_kernel(starts_ref, keys_ref, values_ref, packed_ref):
    packed_ref[0:TOK, 0:HEAD] = keys_ref[...]
    packed_ref[0:TOK, HEAD:] = values_ref[...]
    pos = lax.broadcasted_iota(jnp.int32, (1, TOK), 1)
    owner = jnp.full((1, TOK), -1, jnp.int32)
    for j in range(BEAC):
        owner = owner + (pos >= starts_ref[j]).astype(jnp.int32)
    rows = lax.broadcasted_iota(jnp.int32, (BEAC, TOK), 0)
    member = (rows == owner).astype(F32)
    counts = jnp.sum(member, axis=1, keepdims=True)
    member = member.astype(BF16)
    packed_ref[TOK:, 0:HEAD] = (dot(member, keys_ref[...]) / counts).astype(BF16)
    packed_ref[TOK:, HEAD:] = (dot(member, values_ref[...]) / counts).astype(BF16)


def prep(starts, keys, values):
    return pl.pallas_call(
        prep_kernel,
        out_shape=jax.ShapeDtypeStruct((ROWS, 2 * HEAD), BF16),
        in_specs=[
            pl.BlockSpec(memory_space=pltpu.SMEM),
            whole(TOK, HEAD),
            whole(TOK, HEAD),
        ],
        out_specs=whole(ROWS, 2 * HEAD),
        name="prep",
    )(starts, keys, values)


WIDTH = 1024
GROUPS = HEADS * TOK // WIDTH
COLS = HEADS * TOK
AUG = HEAD + 16
LIMIT = 16 * 2**20
PARAMS = pltpu.CompilerParams(vmem_limit_bytes=LIMIT)
STATE = (
    jax.ShapeDtypeStruct((GROUPS, 1, WIDTH), F32),
    jax.ShapeDtypeStruct((GROUPS, AUG, WIDTH), F32),
)
STATE_SPECS = [whole(GROUPS, 1, WIDTH), whole(GROUPS, AUG, WIDTH)]
QT_SHAPE = jax.ShapeDtypeStruct((GROUPS, HEAD, WIDTH), BF16)
PART = 256


def span(i, width=PART):
    return slice(i * width, (i + 1) * width)


def located(h, part=None):
    if part is None:
        g, at = divmod(h * TOK, WIDTH)
        return g, slice(at, at + TOK)
    g, at = divmod(h * TOK + part * PART, WIDTH)
    return g, slice(at, at + PART)


def local_kernel(queries_ref, block_ref, qt_ref, m_ref, acc_ref, vt_sc):
    vt_sc[0:HEAD, :] = block_ref[0:TOK, HEAD:].T
    vt_sc[HEAD:, :] = jnp.ones((AUG - HEAD, TOK), BF16)
    causal = lax.broadcasted_iota(jnp.int32, (PART, PART), 0) <= lax.broadcasted_iota(
        jnp.int32, (PART, PART), 1
    )
    for h in range(HEADS):
        for part in range(TOK // PART):
            g, at = located(h, part)
            qt = queries_ref[span(part), span(h, HEAD)].T
            qt_ref[g, :, at] = qt
            s = dot(block_ref[span(part), 0:HEAD], qt)
            s = jnp.where(causal, s, -1e30)
            top = jnp.max(s, axis=0, keepdims=True)
            if part:
                past = dot(block_ref[0 : part * PART, 0:HEAD], qt)
                top = jnp.maximum(top, jnp.max(past, axis=0, keepdims=True))
            top = top * C2
            p = jnp.exp2(s * C2 - top).astype(BF16)
            acc = dot(vt_sc[:, span(part)], p)
            if part:
                p = jnp.exp2(past * C2 - top).astype(BF16)
                acc = acc + dot(vt_sc[:, 0 : part * PART], p)
            m_ref[g, :, at] = top
            acc_ref[g, :, at] = acc


def cost(blocks):
    n = HEADS * TOK * TOK * blocks
    return pl.CostEstimate(flops=n * 4 * HEAD, transcendentals=n, bytes_accessed=2**20)


def local(queries, block):
    return pl.pallas_call(
        local_kernel,
        out_shape=(QT_SHAPE, *STATE),
        in_specs=[whole(TOK, HEADS * HEAD), whole(ROWS, 2 * HEAD)],
        out_specs=(whole(GROUPS, HEAD, WIDTH), *STATE_SPECS),
        scratch_shapes=[pltpu.VMEM((AUG, TOK), BF16)],
        cost_estimate=cost(1),
        compiler_params=PARAMS,
        name="local",
    )(queries, block)


def blocks_kernel(places, me_ref, qt_ref, m_in, acc_in, *refs):
    count = len(places)
    me = me_ref[0]
    block_refs = refs[:count]
    m_ref, acc_ref, beacons_ref, k_sc, vt_sc, s_sc, p_sc, top_sc, alpha_sc, index_ref = refs[count:]
    m_ref[...] = m_in[...]
    acc_ref[...] = acc_in[...]
    valid = jnp.int32(0)
    for i in range(count):
        k_sc[i] = block_refs[i][0:TOK, 0:HEAD]
        vt_sc[i, 0:HEAD, :] = block_refs[i][0:TOK, HEAD:].T
        vt_sc[i, HEAD:, :] = jnp.ones((AUG - HEAD, TOK), BF16)
        beacons_ref[i] = block_refs[i][TOK:, :]
        index_ref[valid] = i
        valid = valid + (placed(me, *places[i]) < me).astype(jnp.int32)
    tiles = valid * GROUPS

    def where_is(t):
        return index_ref[t // GROUPS], t % GROUPS

    def score(t):
        i, g = where_is(t)
        s = dot(k_sc[i], qt_ref[g])
        s_sc[...] = s
        top_sc[...] = jnp.max(s, axis=0, keepdims=True) * C2

    def weigh(t):
        i, g = where_is(t)
        old = m_ref[g]
        top = jnp.maximum(old, top_sc[...])
        m_ref[g] = top
        alpha_sc[...] = jnp.exp2(old - top)
        p_sc[...] = jnp.exp2(s_sc[...] * C2 - top).astype(BF16)

    def gather(t):
        i, g = where_is(t)
        acc_ref[g] = acc_ref[g] * alpha_sc[...] + dot(vt_sc[i], p_sc[...])

    def step(t, carry):
        gather(jnp.maximum(t - 1, 0))
        weigh(t)
        score(jnp.minimum(t + 1, tiles - 1))
        return carry

    @pl.when(valid > 0)
    def _():
        p_sc[...] = jnp.zeros_like(p_sc)
        alpha_sc[...] = jnp.ones_like(alpha_sc)
        score(0)
        lax.fori_loop(0, tiles, step, 0)
        gather(tiles - 1)


def attend(me, qt, state, blocks, places):
    count = len(blocks)
    return pl.pallas_call(
        functools.partial(blocks_kernel, places),
        out_shape=(*STATE, jax.ShapeDtypeStruct((count, BEAC, 2 * HEAD), BF16)),
        in_specs=[
            pl.BlockSpec(memory_space=pltpu.SMEM),
            whole(GROUPS, HEAD, WIDTH),
            *STATE_SPECS,
            *[whole(ROWS, 2 * HEAD) for _ in range(count)],
        ],
        out_specs=(*STATE_SPECS, whole(count, BEAC, 2 * HEAD)),
        scratch_shapes=[
            pltpu.VMEM((count, TOK, HEAD), BF16),
            pltpu.VMEM((count, AUG, TOK), BF16),
            pltpu.VMEM((TOK, WIDTH), F32),
            pltpu.VMEM((TOK, WIDTH), BF16),
            pltpu.VMEM((1, WIDTH), F32),
            pltpu.VMEM((1, WIDTH), F32),
            pltpu.SMEM((count + 1,), jnp.int32),
        ],
        cost_estimate=cost(count),
        compiler_params=PARAMS,
        name="attend",
    )(me, qt, *state, *blocks)


def final_kernel(counts, places, me_ref, q_ref, qt_ref, m_loc, acc_loc, acc_ref, *refs):
    beacon_refs = refs[: len(counts)]
    gap_ref, grads_ref, kb_sc, vb_sc = refs[len(counts) :]
    me = me_ref[0]
    kb_sc[...] = jnp.zeros_like(kb_sc)
    vb_sc[...] = jnp.zeros_like(vb_sc)
    n = 0
    for ref, count in zip(beacon_refs, counts):
        for i in range(count):
            at = pl.multiple_of(placed(me, *places[n]) * BEAC, BEAC)
            kb_sc[pl.ds(at, BEAC), :] = ref[i, :, 0:HEAD]
            vb_sc[pl.ds(at, BEAC), :] = ref[i, :, HEAD:]
            n += 1
    kb = kb_sc[...]
    vb = vb_sc[...]
    vbt = vb.T
    seen = lax.broadcasted_iota(jnp.int32, (SEQ * BEAC, TOK), 0) < me * BEAC
    grad_keys = jnp.zeros((SEQ * BEAC, HEAD), F32)
    grad_values = jnp.zeros((SEQ * BEAC, HEAD), F32)
    for h in range(HEADS):
        g, at = located(h)
        s = jnp.where(seen, dot(kb, qt_ref[g, :, at]) * C2, -1e30)
        old = m_loc[g, :, at]
        top = jnp.maximum(old, jnp.max(s, axis=0, keepdims=True))
        alpha = jnp.exp2(old - top)
        p = jnp.exp2(s - top)
        total = acc_loc[g, HEAD : HEAD + 1, at] * alpha + jnp.sum(p, axis=0, keepdims=True)
        inverse = 1.0 / total
        probs = p * inverse
        low = probs.astype(BF16)
        student = acc_loc[g, 0:HEAD, at] * (alpha * inverse) + dot(vbt, low)
        gap_t = (student - acc_ref[g, 0:HEAD, at] * (1.0 / acc_ref[g, HEAD : HEAD + 1, at])).astype(BF16)
        gap = gap_t.T
        gap_ref[:, h * HEAD : (h + 1) * HEAD] = gap
        row_dot = jnp.sum(gap_t.astype(F32) * student, axis=0, keepdims=True)
        score_grad = (probs * (dot(vb, gap_t) - row_dot)).astype(BF16)
        grad_keys = grad_keys + dot(score_grad, q_ref[:, h * HEAD : (h + 1) * HEAD])
        grad_values = grad_values + dot(low, gap)
    grads_ref[:, 0:HEAD] = (grad_keys * SCALE).astype(BF16)
    grads_ref[:, HEAD:] = grad_values.astype(BF16)


def finish(me, queries, qt, state_loc, state, beacons, places):
    counts = [b.shape[0] for b in beacons]
    return pl.pallas_call(
        functools.partial(final_kernel, counts, places),
        out_shape=(
            jax.ShapeDtypeStruct((TOK, HEADS * HEAD), BF16),
            jax.ShapeDtypeStruct((SEQ * BEAC, 2 * HEAD), BF16),
        ),
        in_specs=[
            pl.BlockSpec(memory_space=pltpu.SMEM),
            whole(TOK, HEADS * HEAD),
            whole(GROUPS, HEAD, WIDTH),
            *STATE_SPECS,
            STATE_SPECS[1],
            *[whole(*b.shape) for b in beacons],
        ],
        out_specs=(whole(TOK, HEADS * HEAD), whole(SEQ * BEAC, 2 * HEAD)),
        scratch_shapes=[
            pltpu.VMEM((SEQ * BEAC, HEAD), BF16),
            pltpu.VMEM((SEQ * BEAC, HEAD), BF16),
        ],
        cost_estimate=cost(2),
        compiler_params=PARAMS,
        name="finish",
    )(me, queries, qt, *state_loc, state[1], *beacons)


def moved(block, dx, dy, dc):
    return lax.ppermute(block, "seq", [(s, placed(s, dx, dy, dc)) for s in range(SEQ)])


def body(queries, teacher_keys, teacher_values, beacon_starts):
    me = lax.axis_index("seq").reshape(1)
    own = prep(beacon_starts, teacher_keys, teacher_values)
    left = moved(own, 1, 0, 0)
    right = moved(own, 3, 0, 0)
    across = moved(own, 0, 1, 0)
    twin = moved(own, 0, 0, 1)
    qt, *state_loc = local(queries, own)

    left2 = moved(left, 1, 0, 0)
    right_across = moved(across, 3, 0, 0)
    left_across = moved(left, 0, 1, 0)
    first = [
        (twin, (0, 0, 1)),
        (left, (3, 0, 0)),
        (right, (1, 0, 0)),
        (across, (0, 1, 0)),
        (moved(left, 0, 0, 1), (3, 0, 1)),
        (moved(right, 0, 0, 1), (1, 0, 1)),
        (moved(across, 0, 0, 1), (0, 1, 1)),
    ]
    left2_across = moved(left_across, 1, 0, 0)
    second = [
        (left2, (2, 0, 0)),
        (right_across, (1, 1, 0)),
        (left_across, (3, 1, 0)),
        (moved(left2, 0, 0, 1), (2, 0, 1)),
        (moved(right_across, 0, 0, 1), (1, 1, 1)),
        (moved(left_across, 0, 0, 1), (3, 1, 1)),
    ]
    third = [
        (left2_across, (2, 1, 0)),
        (moved(left2_across, 0, 0, 1), (2, 1, 1)),
    ]
    state = state_loc
    beacons = []
    for stage in (first, second, third):
        blocks, places = zip(*stage)
        *state, rows = attend(me, qt, state, blocks, places)
        beacons.append(rows)
    places = [place for _, place in first + second + third]
    gap, grads = finish(me, queries, qt, state_loc, state, beacons, places)
    arrived = lax.all_to_all(grads.reshape(SEQ, BEAC, 2 * HEAD), "seq", 0, 0, tiled=True)
    total = jnp.sum(arrived.astype(F32), axis=0)
    return gap, total[:, :HEAD], total[:, HEAD:]


def solution(mesh):
    spec = P(("doc", "seq"), None)
    return jax.shard_map(
        body,
        mesh=mesh,
        in_specs=(spec, spec, spec, P(("doc", "seq"))),
        out_specs=(spec, spec, spec),
        check_vma=False,
    )
```

```python
import functools

import jax
import jax.numpy as jnp
from jax import lax
from jax.experimental import pallas as pl
from jax.experimental.pallas import tpu as pltpu
from jax.sharding import PartitionSpec as P


HEADS = 4
HEAD = 128
TOK = 512
BEAC = 32
SEQ = 16
ROWS = TOK + BEAC
SCALE = HEAD**-0.5
LOG2E = 1.4426950408889634
C2 = SCALE * LOG2E
F32 = jnp.float32
BF16 = jnp.bfloat16


def dot(a, b):
    return jnp.dot(a, b, preferred_element_type=F32)


def split_index(s):
    return s // 4, (s // 2) % 2, s % 2


def placed(s, dx, dy, dc):
    x, y, c = split_index(s)
    return ((x + dx) % 4) * 4 + (y + dy) % 2 * 2 + (c + dc) % 2


def whole(*shape):
    return pl.BlockSpec(shape, lambda: tuple(0 for _ in shape))


def prep_kernel(starts_ref, keys_ref, values_ref, packed_ref):
    packed_ref[0:TOK, 0:HEAD] = keys_ref[...]
    packed_ref[0:TOK, HEAD:] = values_ref[...]
    pos = lax.broadcasted_iota(jnp.int32, (1, TOK), 1)
    owner = jnp.full((1, TOK), -1, jnp.int32)
    for j in range(BEAC):
        owner = owner + (pos >= starts_ref[j]).astype(jnp.int32)
    rows = lax.broadcasted_iota(jnp.int32, (BEAC, TOK), 0)
    member = (rows == owner).astype(F32)
    counts = jnp.sum(member, axis=1, keepdims=True)
    member = member.astype(BF16)
    packed_ref[TOK:, 0:HEAD] = (dot(member, keys_ref[...]) / counts).astype(BF16)
    packed_ref[TOK:, HEAD:] = (dot(member, values_ref[...]) / counts).astype(BF16)


def prep(starts, keys, values):
    return pl.pallas_call(
        prep_kernel,
        out_shape=pltpu.VMEM((ROWS, 2 * HEAD), BF16),
        in_specs=[
            pl.BlockSpec(memory_space=pltpu.SMEM),
            whole(TOK, HEAD),
            whole(TOK, HEAD),
        ],
        out_specs=whole(ROWS, 2 * HEAD),
        name="prep",
    )(starts, keys, values)


WIDTH = 1024
GROUPS = HEADS * TOK // WIDTH
AUG = HEAD + 16
SUM = HEAD
TOP = HEAD + 8
PARAMS = pltpu.CompilerParams(vmem_limit_bytes=16 * 2**20)
STATE = jax.ShapeDtypeStruct((GROUPS, AUG, WIDTH), F32)
STATE_SPEC = whole(GROUPS, AUG, WIDTH)
QT_SHAPE = jax.ShapeDtypeStruct((GROUPS, HEAD, WIDTH), BF16)
QT_SPEC = whole(GROUPS, HEAD, WIDTH)
PART = 256


def span(i, width=PART):
    return slice(i * width, (i + 1) * width)


def located(h, part=None):
    if part is None:
        g, at = divmod(h * TOK, WIDTH)
        return g, slice(at, at + TOK)
    g, at = divmod(h * TOK + part * PART, WIDTH)
    return g, slice(at, at + PART)


def local_kernel(queries_ref, keys_ref, values_ref, qt_ref, state_ref, vt_sc):
    vt_sc[0:HEAD, :] = values_ref[...].T
    vt_sc[HEAD:, :] = jnp.ones((AUG - HEAD, TOK), BF16)
    causal = lax.broadcasted_iota(jnp.int32, (PART, PART), 0) <= lax.broadcasted_iota(
        jnp.int32, (PART, PART), 1
    )
    for h in range(HEADS):
        for part in range(TOK // PART):
            g, at = located(h, part)
            qt = queries_ref[span(part), span(h, HEAD)].T
            qt_ref[g, :, at] = qt
            s = dot(keys_ref[span(part), :], qt)
            s = jnp.where(causal, s, -1e30)
            top = jnp.max(s, axis=0, keepdims=True)
            if part:
                past = dot(keys_ref[0 : part * PART, :], qt)
                top = jnp.maximum(top, jnp.max(past, axis=0, keepdims=True))
            top = top * C2
            p = jnp.exp2(s * C2 - top).astype(BF16)
            acc = dot(vt_sc[:, span(part)], p)
            if part:
                p = jnp.exp2(past * C2 - top).astype(BF16)
                acc = acc + dot(vt_sc[:, 0 : part * PART], p)
            state_ref[g, 0:TOP, at] = acc[0:TOP]
            state_ref[g, TOP:, at] = jnp.broadcast_to(top, (AUG - TOP, PART))


def cost(blocks):
    n = HEADS * TOK * TOK * blocks
    return pl.CostEstimate(flops=n * 4 * HEAD, transcendentals=n, bytes_accessed=2**20)


def local(queries, keys, values):
    return pl.pallas_call(
        local_kernel,
        out_shape=(QT_SHAPE, STATE),
        in_specs=[whole(TOK, HEADS * HEAD), whole(TOK, HEAD), whole(TOK, HEAD)],
        out_specs=(QT_SPEC, STATE_SPEC),
        scratch_shapes=[pltpu.VMEM((AUG, TOK), BF16)],
        cost_estimate=cost(1),
        compiler_params=PARAMS,
        name="local",
    )(*[pltpu.with_memory_space_constraint(a, pltpu.HBM) for a in (queries, keys, values)])


def blocks_kernel(sides, start, fresh, pooled, places, me_ref, *refs):
    count = len(places)
    groups = len(sides) * GROUPS
    me = me_ref[0]
    qt_refs, refs = refs[: len(sides)], refs[len(sides) :]
    in_ref, refs = refs[0], refs[1:]
    block_refs, refs = refs[:count], refs[count:]
    acc_ref, refs = refs[0], refs[1:]
    if pooled:
        beacons_ref, refs = refs[0], refs[1:]
    qt_sc, m_sc, k_sc, vt_sc, s_sc, p_sc, top_sc, alpha_sc, tile_ref = refs
    for g in range(groups):
        qt_sc[g] = qt_refs[g // GROUPS][g % GROUPS]
        if g < groups - fresh:
            acc_ref[g] = in_ref[start + g]
            m_sc[g] = in_ref[start + g, TOP : TOP + 1, :]
        else:
            acc_ref[g] = jnp.zeros((AUG, WIDTH), F32)
            m_sc[g] = jnp.full((1, WIDTH), -1e30, F32)
    tiles = jnp.int32(0)
    for i in range(count):
        k_sc[i] = block_refs[i][0:TOK, 0:HEAD]
        vt_sc[i, 0:HEAD, :] = block_refs[i][0:TOK, HEAD:].T
        vt_sc[i, HEAD:, :] = jnp.ones((AUG - HEAD, TOK), BF16)
        if pooled:
            beacons_ref[i] = block_refs[i][TOK:, :]
        for n, side in enumerate(sides):
            seen = (placed(me, *places[i]) < placed(me, 0, 0, side)).astype(jnp.int32)
            for g in range(GROUPS):
                tile_ref[tiles] = i * groups + n * GROUPS + g
                tiles = tiles + seen

    def where_is(t):
        tile = tile_ref[t]
        return tile // groups, tile % groups

    def score(t):
        i, g = where_is(t)
        s = dot(k_sc[i], qt_sc[g])
        s_sc[...] = s
        top_sc[...] = jnp.max(s, axis=0, keepdims=True) * C2

    def weigh(t):
        _, g = where_is(t)
        old = m_sc[g]
        top = jnp.maximum(old, top_sc[...])
        m_sc[g] = top
        alpha_sc[...] = jnp.exp2(old - top)
        p_sc[...] = jnp.exp2(s_sc[...] * C2 - top).astype(BF16)

    def gather(t):
        i, g = where_is(t)
        acc_ref[g] = acc_ref[g] * alpha_sc[...] + dot(vt_sc[i], p_sc[...])

    def step(t, carry):
        gather(jnp.maximum(t - 1, 0))
        weigh(t)
        score(jnp.minimum(t + 1, tiles - 1))
        return carry

    @pl.when(tiles > 0)
    def _():
        p_sc[...] = jnp.zeros_like(p_sc)
        alpha_sc[...] = jnp.ones_like(alpha_sc)
        score(0)
        lax.fori_loop(0, tiles, step, 0)
        gather(tiles - 1)

    for g in range(groups):
        acc_ref[g, TOP:] = jnp.broadcast_to(m_sc[g], (AUG - TOP, WIDTH))


def attend(me, sides, qts, state, blocks, places, start=0, fresh=0, pooled=1):
    count, groups = len(blocks), len(sides) * GROUPS
    return pl.pallas_call(
        functools.partial(blocks_kernel, sides, start, fresh, pooled, places),
        out_shape=(
            jax.ShapeDtypeStruct((groups, AUG, WIDTH), F32),
            *[jax.ShapeDtypeStruct((count, BEAC, 2 * HEAD), BF16)] * pooled,
        ),
        in_specs=[
            pl.BlockSpec(memory_space=pltpu.SMEM),
            *[QT_SPEC] * len(sides),
            whole(*state.shape),
            *[whole(ROWS, 2 * HEAD)] * count,
        ],
        out_specs=(whole(groups, AUG, WIDTH), *[whole(count, BEAC, 2 * HEAD)] * pooled),
        scratch_shapes=[
            pltpu.VMEM((groups, HEAD, WIDTH), BF16),
            pltpu.VMEM((groups, 1, WIDTH), F32),
            pltpu.VMEM((count, TOK, HEAD), BF16),
            pltpu.VMEM((count, AUG, TOK), BF16),
            pltpu.VMEM((TOK, WIDTH), F32),
            pltpu.VMEM((TOK, WIDTH), BF16),
            pltpu.VMEM((1, WIDTH), F32),
            pltpu.VMEM((1, WIDTH), F32),
            pltpu.SMEM((count * groups + 1,), jnp.int32),
        ],
        cost_estimate=cost(count * len(sides)),
        compiler_params=PARAMS,
        name="attend",
    )(me, *qts, state, *blocks)


def final_kernel(counts, places, me_ref, q_ref, qt_ref, local_ref, mine_ref, sent_ref, *refs):
    beacon_refs = refs[: len(counts)]
    gap_ref, grads_ref, kb_sc, vb_sc, vt_sc, s_sc, p_sc, grad_sc, gap_sc = refs[len(counts) :]
    me = me_ref[0]
    kb_sc[...] = jnp.zeros_like(kb_sc)
    vb_sc[...] = jnp.zeros_like(vb_sc)
    n = 0
    for ref, count in zip(beacon_refs, counts):
        for i in range(count):
            at = pl.multiple_of(placed(me, *places[n]) * BEAC, BEAC)
            kb_sc[pl.ds(at, BEAC), :] = ref[i, :, 0:HEAD]
            vb_sc[pl.ds(at, BEAC), :] = ref[i, :, HEAD:]
            n += 1
    kb = kb_sc[...]
    vb = vb_sc[...]
    vt_sc[0:HEAD, :] = vb.T
    vt_sc[HEAD:, :] = jnp.ones((AUG - HEAD, SEQ * BEAC), BF16)
    seen = lax.broadcasted_iota(jnp.int32, (SEQ * BEAC, TOK), 0) < me * BEAC
    tops = []
    for h in range(HEADS):
        g, at = located(h)
        s = jnp.where(seen, dot(kb, qt_ref[g, :, at]), -1e30)
        s_sc[h] = s
        old = local_ref[g, TOP : TOP + 1, at]
        tops.append(jnp.maximum(old, jnp.max(s, axis=0, keepdims=True) * C2))
    for h in range(HEADS):
        p_sc[h] = jnp.exp2(s_sc[h] * C2 - tops[h]).astype(BF16)
    scaled = []
    for h in range(HEADS):
        g, at = located(h)
        old = jnp.exp2(local_ref[g, TOP : TOP + 1, at] - tops[h])
        student = local_ref[g, :, at] * old + dot(vt_sc[...], p_sc[h])
        inverse = 1.0 / student[SUM : SUM + 1, :]
        student = student[0:HEAD, :] * inverse
        old, new = mine_ref[g, TOP : TOP + 1, at], sent_ref[g, TOP : TOP + 1, at]
        top = jnp.maximum(old, new)
        old, new = jnp.exp2(old - top), jnp.exp2(new - top)
        total = mine_ref[g, SUM : SUM + 1, at] * old + sent_ref[g, SUM : SUM + 1, at] * new
        total = 1.0 / total
        teacher = mine_ref[g, 0:HEAD, at] * (old * total) + sent_ref[g, 0:HEAD, at] * (new * total)
        gap_t = (student - teacher).astype(BF16)
        gap_ref[:, span(h, HEAD)] = gap_t.T
        gap_t = gap_t.astype(F32) * inverse
        row_dot = jnp.sum(gap_t * student, axis=0, keepdims=True)
        gap_t = gap_t.astype(BF16)
        gap_sc[h] = gap_t.T
        scaled.append((gap_t, row_dot))
    for h in range(HEADS):
        gap_t, row_dot = scaled[h]
        grad_sc[h] = (p_sc[h].astype(F32) * (dot(vb, gap_t) - row_dot)).astype(BF16)
    grad_keys = dot(grad_sc[0], q_ref[:, span(0, HEAD)])
    grad_values = dot(p_sc[0], gap_sc[0])
    for h in range(1, HEADS):
        grad_keys = grad_keys + dot(grad_sc[h], q_ref[:, span(h, HEAD)])
        grad_values = grad_values + dot(p_sc[h], gap_sc[h])
    grads_ref[:, 0:HEAD] = (grad_keys * SCALE).astype(BF16)
    grads_ref[:, HEAD:] = grad_values.astype(BF16)


def finish(me, queries, qt, states, beacons, places):
    counts = [b.shape[0] for b in beacons]
    return pl.pallas_call(
        functools.partial(final_kernel, counts, places),
        out_shape=(
            jax.ShapeDtypeStruct((TOK, HEADS * HEAD), BF16),
            jax.ShapeDtypeStruct((SEQ * BEAC, 2 * HEAD), BF16),
        ),
        in_specs=[
            pl.BlockSpec(memory_space=pltpu.SMEM),
            whole(TOK, HEADS * HEAD),
            QT_SPEC,
            *[STATE_SPEC] * len(states),
            *[whole(*b.shape) for b in beacons],
        ],
        out_specs=(whole(TOK, HEADS * HEAD), whole(SEQ * BEAC, 2 * HEAD)),
        scratch_shapes=[
            pltpu.VMEM((SEQ * BEAC, HEAD), BF16),
            pltpu.VMEM((SEQ * BEAC, HEAD), BF16),
            pltpu.VMEM((AUG, SEQ * BEAC), BF16),
            pltpu.VMEM((HEADS, SEQ * BEAC, TOK), F32),
            pltpu.VMEM((HEADS, SEQ * BEAC, TOK), BF16),
            pltpu.VMEM((HEADS, SEQ * BEAC, TOK), BF16),
            pltpu.VMEM((HEADS, TOK, HEAD), BF16),
        ],
        cost_estimate=cost(2),
        compiler_params=PARAMS,
        name="finish",
    )(me, queries, qt, *states, *beacons)


def moved(block, dx, dy, dc):
    return lax.ppermute(block, "seq", [(s, placed(s, dx, dy, dc)) for s in range(SEQ)])


def swapped(block):
    return moved(block, 0, 0, 1)


def layer(queries, teacher_keys, teacher_values, beacon_starts):
    me = lax.axis_index("seq").reshape(1)
    own = prep(beacon_starts, teacher_keys, teacher_values)
    left = moved(own, 1, 0, 0)
    across = moved(own, 0, 1, 0)
    right = moved(own, 3, 0, 0)
    qt, state_local = local(queries, teacher_keys, teacher_values)
    qt_twin = swapped(qt)
    opposite = moved(own, 2, 1, 0)
    left2 = moved(left, 1, 0, 0)
    left_across = moved(left, 0, 1, 0)
    right_across = moved(across, 3, 0, 0)
    near = [own, left, across, right]
    near_places = [(0, 0, 0), (3, 0, 0), (0, 1, 0), (1, 0, 0)]
    far = [left2, left_across, right_across, opposite]
    far_places = [(2, 0, 0), (3, 1, 0), (1, 1, 0), (2, 1, 0)]
    state, near_rows = attend(
        me, (0, 1), (qt, qt_twin), state_local, near, near_places, fresh=GROUPS
    )
    near_twin = swapped(near_rows)
    lent, far_rows = attend(me, (1,), (qt_twin,), state, far, far_places, start=GROUPS)
    sent = swapped(lent)
    far_twin = swapped(far_rows)
    (mine,) = attend(me, (0,), (qt,), state, far, far_places, pooled=0)
    places = near_places + far_places
    places = places + [(dx, dy, 1) for dx, dy, _ in places]
    gap, grads = finish(
        me,
        queries,
        qt,
        (state_local, mine, sent),
        (near_rows, far_rows, near_twin, far_twin),
        places,
    )
    arrived = lax.all_to_all(grads.reshape(SEQ, BEAC, 2 * HEAD), "seq", 0, 0, tiled=True)
    key_rows, value_rows = (
        jnp.sum(part.astype(F32), axis=0) for part in jnp.split(arrived, 2, axis=2)
    )
    return gap, key_rows, value_rows


def solution(mesh):
    spec = P(("doc", "seq"), None)
    return jax.shard_map(
        layer,
        mesh=mesh,
        in_specs=(spec, spec, spec, P(("doc", "seq"))),
        out_specs=(spec, spec, spec),
        check_vma=False,
    )
```

```python
import functools

import jax
import jax.numpy as jnp
from jax import lax
from jax.experimental import pallas as pl
from jax.experimental.pallas import tpu as pltpu
from jax.sharding import PartitionSpec as P


HEADS = 4
HEAD = 128
TOK = 512
BEAC = 32
SEQ = 16
ROWS = TOK + BEAC
SCALE = HEAD**-0.5
LOG2E = 1.4426950408889634
C2 = SCALE * LOG2E
F32 = jnp.float32
BF16 = jnp.bfloat16


def dot(a, b):
    return jnp.dot(a, b, preferred_element_type=F32)


def split_index(s):
    return s // 4, (s // 2) % 2, s % 2


def placed(s, dx, dy, dc):
    x, y, c = split_index(s)
    return ((x + dx) % 4) * 4 + (y + dy) % 2 * 2 + (c + dc) % 2


def whole(*shape):
    return pl.BlockSpec(shape, lambda: tuple(0 for _ in shape))


def prep_kernel(starts_ref, keys_ref, values_ref, packed_ref):
    packed_ref[0:TOK, 0:HEAD] = keys_ref[...]
    packed_ref[0:TOK, HEAD:] = values_ref[...]
    pos = lax.broadcasted_iota(jnp.int32, (1, TOK), 1)
    owner = jnp.full((1, TOK), -1, jnp.int32)
    for j in range(BEAC):
        owner = owner + (pos >= starts_ref[j]).astype(jnp.int32)
    rows = lax.broadcasted_iota(jnp.int32, (BEAC, TOK), 0)
    member = (rows == owner).astype(F32)
    counts = jnp.sum(member, axis=1, keepdims=True)
    member = member.astype(BF16)
    packed_ref[TOK:, 0:HEAD] = (dot(member, keys_ref[...]) / counts).astype(BF16)
    packed_ref[TOK:, HEAD:] = (dot(member, values_ref[...]) / counts).astype(BF16)


def prep(starts, keys, values):
    return pl.pallas_call(
        prep_kernel,
        out_shape=pltpu.VMEM((ROWS, 2 * HEAD), BF16),
        in_specs=[
            pl.BlockSpec(memory_space=pltpu.SMEM),
            whole(TOK, HEAD),
            whole(TOK, HEAD),
        ],
        out_specs=whole(ROWS, 2 * HEAD),
        name="prep",
    )(starts, keys, values)


WIDTH = 1024
GROUPS = HEADS * TOK // WIDTH
AUG = HEAD + 16
SUM = HEAD
TOP = HEAD + 8
PARAMS = pltpu.CompilerParams(vmem_limit_bytes=16 * 2**20)
STATE = jax.ShapeDtypeStruct((GROUPS, AUG, WIDTH), F32)
STATE_SPEC = whole(GROUPS, AUG, WIDTH)
QT_SHAPE = jax.ShapeDtypeStruct((GROUPS, HEAD, WIDTH), BF16)
QT_SPEC = whole(GROUPS, HEAD, WIDTH)
PART = 256


def span(i, width=PART):
    return slice(i * width, (i + 1) * width)


def located(h, part=None):
    if part is None:
        g, at = divmod(h * TOK, WIDTH)
        return g, slice(at, at + TOK)
    g, at = divmod(h * TOK + part * PART, WIDTH)
    return g, slice(at, at + PART)


def local_kernel(queries_ref, keys_ref, values_ref, qt_ref, state_ref, vt_sc):
    vt_sc[0:HEAD, :] = values_ref[...].T
    vt_sc[HEAD:, :] = jnp.ones((AUG - HEAD, TOK), BF16)
    causal = lax.broadcasted_iota(jnp.int32, (PART, PART), 0) <= lax.broadcasted_iota(
        jnp.int32, (PART, PART), 1
    )
    for h in range(HEADS):
        for part in range(TOK // PART):
            g, at = located(h, part)
            qt = queries_ref[span(part), span(h, HEAD)].T
            qt_ref[g, :, at] = qt
            s = dot(keys_ref[span(part), :], qt)
            s = jnp.where(causal, s, -1e30)
            top = jnp.max(s, axis=0, keepdims=True)
            if part:
                past = dot(keys_ref[0 : part * PART, :], qt)
                top = jnp.maximum(top, jnp.max(past, axis=0, keepdims=True))
            top = top * C2
            p = jnp.exp2(s * C2 - top).astype(BF16)
            acc = dot(vt_sc[:, span(part)], p)
            if part:
                p = jnp.exp2(past * C2 - top).astype(BF16)
                acc = acc + dot(vt_sc[:, 0 : part * PART], p)
            state_ref[g, 0:TOP, at] = acc[0:TOP]
            state_ref[g, TOP:, at] = jnp.broadcast_to(top, (AUG - TOP, PART))


def cost(blocks):
    n = HEADS * TOK * TOK * blocks
    return pl.CostEstimate(flops=n * 4 * HEAD, transcendentals=n, bytes_accessed=2**20)


def local(queries, keys, values):
    return pl.pallas_call(
        local_kernel,
        out_shape=(QT_SHAPE, STATE),
        in_specs=[whole(TOK, HEADS * HEAD), whole(TOK, HEAD), whole(TOK, HEAD)],
        out_specs=(QT_SPEC, STATE_SPEC),
        scratch_shapes=[pltpu.VMEM((AUG, TOK), BF16)],
        cost_estimate=cost(1),
        compiler_params=PARAMS,
        name="local",
    )(*[pltpu.with_memory_space_constraint(a, pltpu.HBM) for a in (queries, keys, values)])


def blocks_kernel(sides, start, fresh, pooled, places, *refs):
    count = len(places)
    groups = len(sides) * GROUPS
    me = lax.axis_index("seq")
    qt_refs, refs = refs[: len(sides)], refs[len(sides) :]
    in_ref, refs = refs[0], refs[1:]
    block_refs, refs = refs[:count], refs[count:]
    acc_ref, refs = refs[0], refs[1:]
    if pooled:
        beacons_ref, refs = refs[0], refs[1:]
    qt_sc, m_sc, k_sc, vt_sc, s_sc, p_sc, top_sc, alpha_sc, tile_ref = refs
    for g in range(groups):
        qt_sc[g] = qt_refs[g // GROUPS][g % GROUPS]
        if g < groups - fresh:
            acc_ref[g] = in_ref[start + g]
            m_sc[g] = in_ref[start + g, TOP : TOP + 1, :]
        else:
            acc_ref[g] = jnp.zeros((AUG, WIDTH), F32)
            m_sc[g] = jnp.full((1, WIDTH), -1e30, F32)
    tiles = jnp.int32(0)
    for i in range(count):
        for n, side in enumerate(sides):
            seen = (placed(me, *places[i]) < placed(me, 0, 0, side)).astype(jnp.int32)
            for g in range(GROUPS):
                tile_ref[tiles] = i * groups + n * GROUPS + g
                tiles = tiles + seen
        k_sc[i] = block_refs[i][0:TOK, 0:HEAD]

    def where_is(t):
        tile = tile_ref[t]
        return tile // groups, tile % groups

    def score(t):
        i, g = where_is(t)
        s = dot(k_sc[i], qt_sc[g])
        s_sc[...] = s
        top_sc[...] = jnp.max(s, axis=0, keepdims=True) * C2

    def weigh(t):
        _, g = where_is(t)
        old = m_sc[g]
        top = jnp.maximum(old, top_sc[...])
        m_sc[g] = top
        alpha_sc[...] = jnp.exp2(old - top)
        p_sc[...] = jnp.exp2(s_sc[...] * C2 - top).astype(BF16)

    def gather(t):
        i, g = where_is(t)
        acc_ref[g] = acc_ref[g] * alpha_sc[...] + dot(vt_sc[i], p_sc[...])

    def step(t, carry):
        gather(t - 1)
        weigh(t)
        score(jnp.minimum(t + 1, tiles - 1))
        return carry

    score(0)
    for i in range(count):
        vt_sc[i, 0:HEAD, :] = block_refs[i][0:TOK, HEAD:].T
        vt_sc[i, HEAD:, :] = jnp.ones((AUG - HEAD, TOK), BF16)
        if pooled:
            beacons_ref[i] = block_refs[i][TOK:, :]

    @pl.when(tiles > 0)
    def _():
        weigh(0)
        score(1)
        lax.fori_loop(1, tiles, step, 0)
        gather(tiles - 1)

    for g in range(groups):
        acc_ref[g, TOP:] = jnp.broadcast_to(m_sc[g], (AUG - TOP, WIDTH))


def attend(sides, qts, state, blocks, places, start=0, fresh=0, pooled=1):
    count, groups = len(blocks), len(sides) * GROUPS
    return pl.pallas_call(
        functools.partial(blocks_kernel, sides, start, fresh, pooled, places),
        out_shape=(
            jax.ShapeDtypeStruct((groups, AUG, WIDTH), F32),
            *[jax.ShapeDtypeStruct((count, BEAC, 2 * HEAD), BF16)] * pooled,
        ),
        in_specs=[
            *[QT_SPEC] * len(sides),
            whole(*state.shape),
            *[whole(ROWS, 2 * HEAD)] * count,
        ],
        out_specs=(whole(groups, AUG, WIDTH), *[whole(count, BEAC, 2 * HEAD)] * pooled),
        scratch_shapes=[
            pltpu.VMEM((groups, HEAD, WIDTH), BF16),
            pltpu.VMEM((groups, 1, WIDTH), F32),
            pltpu.VMEM((count, TOK, HEAD), BF16),
            pltpu.VMEM((count, AUG, TOK), BF16),
            pltpu.VMEM((TOK, WIDTH), F32),
            pltpu.VMEM((TOK, WIDTH), BF16),
            pltpu.VMEM((1, WIDTH), F32),
            pltpu.VMEM((1, WIDTH), F32),
            pltpu.SMEM((count * groups + 1,), jnp.int32),
        ],
        cost_estimate=cost(count * len(sides)),
        compiler_params=PARAMS,
        name="attend",
    )(*qts, state, *blocks)


def final_kernel(counts, places, q_ref, qt_ref, local_ref, mine_ref, sent_ref, *refs):
    beacon_refs = refs[: len(counts)]
    gap_hbm, grads_ref, gap_ref, kb_sc, vb_sc, vt_sc, s_sc, p_sc, grad_sc, gap_sc, sem = refs[len(counts) :]
    me = lax.axis_index("seq")
    kb_sc[...] = jnp.zeros_like(kb_sc)
    vb_sc[...] = jnp.zeros_like(vb_sc)
    n = 0
    for ref, count in zip(beacon_refs, counts):
        for i in range(count):
            at = pl.multiple_of(placed(me, *places[n]) * BEAC, BEAC)
            kb_sc[pl.ds(at, BEAC), :] = ref[i, :, 0:HEAD]
            vb_sc[pl.ds(at, BEAC), :] = ref[i, :, HEAD:]
            n += 1
    kb = kb_sc[...]
    vb = vb_sc[...]
    vt_sc[0:HEAD, :] = vb.T
    vt_sc[HEAD:, :] = jnp.ones((AUG - HEAD, SEQ * BEAC), BF16)
    seen = lax.broadcasted_iota(jnp.int32, (SEQ * BEAC, TOK), 0) < me * BEAC
    tops = []
    for h in range(HEADS):
        g, at = located(h)
        s = jnp.where(seen, dot(kb, qt_ref[g, :, at]), -1e30)
        s_sc[h] = s
        old = local_ref[g, TOP : TOP + 1, at]
        tops.append(jnp.maximum(old, jnp.max(s, axis=0, keepdims=True) * C2))
    for h in range(HEADS):
        p_sc[h] = jnp.exp2(s_sc[h] * C2 - tops[h]).astype(BF16)
    scaled = []
    for h in range(HEADS):
        g, at = located(h)
        old = jnp.exp2(local_ref[g, TOP : TOP + 1, at] - tops[h])
        student = local_ref[g, :, at] * old + dot(vt_sc[...], p_sc[h])
        inverse = 1.0 / student[SUM : SUM + 1, :]
        student = student[0:HEAD, :] * inverse
        old, new = mine_ref[g, TOP : TOP + 1, at], sent_ref[g, TOP : TOP + 1, at]
        top = jnp.maximum(old, new)
        old, new = jnp.exp2(old - top), jnp.exp2(new - top)
        total = mine_ref[g, SUM : SUM + 1, at] * old + sent_ref[g, SUM : SUM + 1, at] * new
        total = 1.0 / total
        teacher = mine_ref[g, 0:HEAD, at] * (old * total) + sent_ref[g, 0:HEAD, at] * (new * total)
        gap_t = (student - teacher).astype(BF16)
        gap_ref[:, span(h, HEAD)] = gap_t.T
        gap_t = gap_t.astype(F32) * inverse
        row_dot = jnp.sum(gap_t * student, axis=0, keepdims=True)
        gap_t = gap_t.astype(BF16)
        gap_sc[h] = gap_t.T
        scaled.append((gap_t, row_dot))
    gap_copy = pltpu.make_async_copy(gap_ref, gap_hbm, sem)
    gap_copy.start()
    for h in range(HEADS):
        gap_t, row_dot = scaled[h]
        grad_sc[h] = (p_sc[h].astype(F32) * (dot(vb, gap_t) - row_dot)).astype(BF16)
    grad_keys = dot(grad_sc[0], q_ref[:, span(0, HEAD)])
    grad_values = dot(p_sc[0], gap_sc[0])
    for h in range(1, HEADS):
        grad_keys = grad_keys + dot(grad_sc[h], q_ref[:, span(h, HEAD)])
        grad_values = grad_values + dot(p_sc[h], gap_sc[h])
    grads_ref[:, 0:HEAD] = (grad_keys * SCALE).astype(BF16)
    grads_ref[:, HEAD:] = grad_values.astype(BF16)
    gap_copy.wait()


def finish(queries, qt, states, beacons, places):
    counts = [b.shape[0] for b in beacons]
    return pl.pallas_call(
        functools.partial(final_kernel, counts, places),
        out_shape=(
            jax.ShapeDtypeStruct((TOK, HEADS * HEAD), BF16),
            pltpu.VMEM((SEQ * BEAC, 2 * HEAD), BF16),
        ),
        in_specs=[
            whole(TOK, HEADS * HEAD),
            QT_SPEC,
            *[STATE_SPEC] * len(states),
            *[whole(*b.shape) for b in beacons],
        ],
        out_specs=(pl.BlockSpec(memory_space=pl.ANY), whole(SEQ * BEAC, 2 * HEAD)),
        scratch_shapes=[
            pltpu.VMEM((TOK, HEADS * HEAD), BF16),
            pltpu.VMEM((SEQ * BEAC, HEAD), BF16),
            pltpu.VMEM((SEQ * BEAC, HEAD), BF16),
            pltpu.VMEM((AUG, SEQ * BEAC), BF16),
            pltpu.VMEM((HEADS, SEQ * BEAC, TOK), F32),
            pltpu.VMEM((HEADS, SEQ * BEAC, TOK), BF16),
            pltpu.VMEM((HEADS, SEQ * BEAC, TOK), BF16),
            pltpu.VMEM((HEADS, TOK, HEAD), BF16),
            pltpu.SemaphoreType.DMA,
        ],
        cost_estimate=cost(2),
        compiler_params=PARAMS,
        name="finish",
    )(queries, qt, *states, *beacons)


def moved(block, dx, dy, dc):
    return lax.ppermute(block, "seq", [(s, placed(s, dx, dy, dc)) for s in range(SEQ)])


def swapped(block):
    return moved(block, 0, 0, 1)


def layer(queries, teacher_keys, teacher_values, beacon_starts):
    own = prep(beacon_starts, teacher_keys, teacher_values)
    left = moved(own, 1, 0, 0)
    across = moved(own, 0, 1, 0)
    right = moved(own, 3, 0, 0)
    qt, state_local = local(queries, teacher_keys, teacher_values)
    qt_twin = swapped(qt)
    opposite = moved(own, 2, 1, 0)
    left2 = moved(left, 1, 0, 0)
    left_across = moved(left, 0, 1, 0)
    right_across = moved(across, 3, 0, 0)
    near = [own, left, across, right]
    near_places = [(0, 0, 0), (3, 0, 0), (0, 1, 0), (1, 0, 0)]
    far = [left2, left_across, right_across, opposite]
    far_places = [(2, 0, 0), (3, 1, 0), (1, 1, 0), (2, 1, 0)]
    state, near_rows = attend(
        (0, 1), (qt, qt_twin), state_local, near, near_places, fresh=GROUPS
    )
    near_twin = swapped(near_rows)
    lent, far_rows = attend((1,), (qt_twin,), state, far, far_places, start=GROUPS)
    sent = swapped(lent)
    far_twin = swapped(far_rows)
    (mine,) = attend((0,), (qt,), state, far, far_places, pooled=0)
    places = near_places + far_places
    places = places + [(dx, dy, 1) for dx, dy, _ in places]
    gap, grads = finish(
        queries,
        qt,
        (state_local, mine, sent),
        (near_rows, far_rows, near_twin, far_twin),
        places,
    )
    arrived = lax.all_to_all(grads.reshape(SEQ, BEAC, 2 * HEAD), "seq", 0, 0, tiled=True)
    key_rows, value_rows = (
        jnp.sum(part.astype(F32), axis=0) for part in jnp.split(arrived, 2, axis=2)
    )
    return gap, key_rows, value_rows


def solution(mesh):
    spec = P(("doc", "seq"), None)
    return jax.shard_map(
        layer,
        mesh=mesh,
        in_specs=(spec, spec, spec, P(("doc", "seq"))),
        out_specs=(spec, spec, spec),
        check_vma=False,
    )
```

```python
import functools

import jax
import jax.numpy as jnp
from jax import lax
from jax.experimental import pallas as pl
from jax.experimental.pallas import tpu as pltpu
from jax.sharding import PartitionSpec as P


HEADS = 4
HEAD = 128
TOK = 512
BEAC = 32
SEQ = 16
ROWS = TOK + BEAC
SCALE = HEAD**-0.5
LOG2E = 1.4426950408889634
C2 = SCALE * LOG2E
F32 = jnp.float32
BF16 = jnp.bfloat16


def dot(a, b):
    return jnp.dot(a, b, preferred_element_type=F32)


def split_index(s):
    return s // 4, (s // 2) % 2, s % 2


def placed(s, dx, dy, dc):
    x, y, c = split_index(s)
    return ((x + dx) % 4) * 4 + (y + dy) % 2 * 2 + (c + dc) % 2


def whole(*shape):
    return pl.BlockSpec(shape, lambda: tuple(0 for _ in shape))


def prep_kernel(starts_ref, keys_ref, values_ref, packed_ref):
    packed_ref[0:TOK, 0:HEAD] = keys_ref[...]
    packed_ref[0:TOK, HEAD:] = values_ref[...]
    pos = lax.broadcasted_iota(jnp.int32, (1, TOK), 1)
    owner = jnp.full((1, TOK), -1, jnp.int32)
    for j in range(BEAC):
        owner = owner + (pos >= starts_ref[j]).astype(jnp.int32)
    rows = lax.broadcasted_iota(jnp.int32, (BEAC, TOK), 0)
    member = (rows == owner).astype(F32)
    counts = jnp.sum(member, axis=1, keepdims=True)
    member = member.astype(BF16)
    packed_ref[TOK:, 0:HEAD] = (dot(member, keys_ref[...]) / counts).astype(BF16)
    packed_ref[TOK:, HEAD:] = (dot(member, values_ref[...]) / counts).astype(BF16)


def prep(starts, keys, values):
    return pl.pallas_call(
        prep_kernel,
        out_shape=pltpu.VMEM((ROWS, 2 * HEAD), BF16),
        in_specs=[
            pl.BlockSpec(memory_space=pltpu.SMEM),
            whole(TOK, HEAD),
            whole(TOK, HEAD),
        ],
        out_specs=whole(ROWS, 2 * HEAD),
        name="prep",
    )(starts, keys, values)


WIDTH = 1024
GROUPS = HEADS * TOK // WIDTH
AUG = HEAD + 16
SUM = HEAD
TOP = HEAD + 8
PARAMS = pltpu.CompilerParams(vmem_limit_bytes=16 * 2**20)
STATE = jax.ShapeDtypeStruct((GROUPS, AUG, WIDTH), F32)
STATE_SPEC = whole(GROUPS, AUG, WIDTH)
QT_SHAPE = jax.ShapeDtypeStruct((GROUPS, HEAD, WIDTH), BF16)
QT_SPEC = whole(GROUPS, HEAD, WIDTH)
PART = 256


def span(i, width=PART):
    return slice(i * width, (i + 1) * width)


def located(h, part=None):
    if part is None:
        g, at = divmod(h * TOK, WIDTH)
        return g, slice(at, at + TOK)
    g, at = divmod(h * TOK + part * PART, WIDTH)
    return g, slice(at, at + PART)


def local_kernel(queries_ref, keys_ref, values_ref, qt_ref, state_ref, vt_sc):
    vt_sc[0:HEAD, :] = values_ref[...].T
    vt_sc[HEAD:, :] = jnp.ones((AUG - HEAD, TOK), BF16)
    causal = lax.broadcasted_iota(jnp.int32, (PART, PART), 0) <= lax.broadcasted_iota(
        jnp.int32, (PART, PART), 1
    )
    for h in range(HEADS):
        for part in range(TOK // PART):
            g, at = located(h, part)
            qt = queries_ref[span(part), span(h, HEAD)].T
            qt_ref[g, :, at] = qt
            s = dot(keys_ref[span(part), :], qt)
            s = jnp.where(causal, s, -1e30)
            top = jnp.max(s, axis=0, keepdims=True)
            if part:
                past = dot(keys_ref[0 : part * PART, :], qt)
                top = jnp.maximum(top, jnp.max(past, axis=0, keepdims=True))
            top = top * C2
            p = jnp.exp2(s * C2 - top).astype(BF16)
            acc = dot(vt_sc[:, span(part)], p)
            if part:
                p = jnp.exp2(past * C2 - top).astype(BF16)
                acc = acc + dot(vt_sc[:, 0 : part * PART], p)
            state_ref[g, 0:TOP, at] = acc[0:TOP]
            state_ref[g, TOP:, at] = jnp.broadcast_to(top, (AUG - TOP, PART))


def cost(blocks):
    n = HEADS * TOK * TOK * blocks
    return pl.CostEstimate(flops=n * 4 * HEAD, transcendentals=n, bytes_accessed=2**20)


def local(queries, keys, values):
    return pl.pallas_call(
        local_kernel,
        out_shape=(QT_SHAPE, STATE),
        in_specs=[whole(TOK, HEADS * HEAD), whole(TOK, HEAD), whole(TOK, HEAD)],
        out_specs=(QT_SPEC, STATE_SPEC),
        scratch_shapes=[pltpu.VMEM((AUG, TOK), BF16)],
        cost_estimate=cost(1),
        compiler_params=PARAMS,
        name="local",
    )(*[pltpu.with_memory_space_constraint(a, pltpu.HBM) for a in (queries, keys, values)])


def blocks_kernel(sides, start, fresh, pooled, before, places, *refs):
    count = len(places)
    groups = len(sides) * GROUPS
    me = lax.axis_index("seq")
    qt_refs, refs = refs[: len(sides)], refs[len(sides) :]
    in_ref, refs = refs[0], refs[1:]
    block_refs, refs = refs[:count], refs[count:]
    if before:
        before_ref, refs = refs[0], refs[1:]
    acc_ref, refs = refs[0], refs[1:]
    if pooled:
        beacons_ref, refs = refs[0], refs[1:]
    qt_sc, m_sc, k_sc, vt_sc, s_sc, p_sc, top_sc, alpha_sc, tile_ref = refs
    for g in range(groups):
        qt_sc[g] = qt_refs[g // GROUPS][g % GROUPS]
        if g < groups - fresh:
            acc_ref[g] = in_ref[start + g]
            m_sc[g] = in_ref[start + g, TOP : TOP + 1, :]
        else:
            acc_ref[g] = jnp.zeros((AUG, WIDTH), F32)
            m_sc[g] = jnp.full((1, WIDTH), -1e30, F32)
    tiles = jnp.int32(0)
    for i in range(count):
        for n, side in enumerate(sides):
            seen = (placed(me, *places[i]) < placed(me, 0, 0, side)).astype(jnp.int32)
            for g in range(GROUPS):
                tile_ref[tiles] = i * groups + n * GROUPS + g
                tiles = tiles + seen
        k_sc[i] = block_refs[i][0:TOK, 0:HEAD]

    def where_is(t):
        tile = tile_ref[t]
        return tile // groups, tile % groups

    def score(t):
        i, g = where_is(t)
        s = dot(k_sc[i], qt_sc[g])
        s_sc[...] = s
        top_sc[...] = jnp.max(s, axis=0, keepdims=True) * C2

    def weigh(t):
        _, g = where_is(t)
        old = m_sc[g]
        top = jnp.maximum(old, top_sc[...])
        m_sc[g] = top
        alpha_sc[...] = jnp.exp2(old - top)
        p_sc[...] = jnp.exp2(s_sc[...] * C2 - top).astype(BF16)

    def gather(t):
        i, g = where_is(t)
        acc_ref[g] = acc_ref[g] * alpha_sc[...] + dot(vt_sc[i], p_sc[...])

    def step(t, carry):
        gather(t - 1)
        weigh(t)
        score(jnp.minimum(t + 1, tiles - 1))
        return carry

    score(0)
    for i in range(count):
        vt_sc[i, 0:HEAD, :] = block_refs[i][0:TOK, HEAD:].T
        vt_sc[i, HEAD:, :] = jnp.ones((AUG - HEAD, TOK), BF16)
        if pooled:
            beacons_ref[before + i] = block_refs[i][TOK:, :]
    if before:
        beacons_ref[0:before] = before_ref[...]

    @pl.when(tiles > 0)
    def _():
        weigh(0)
        score(1)
        lax.fori_loop(1, tiles, step, 0)
        gather(tiles - 1)

    for g in range(groups):
        acc_ref[g, TOP:] = jnp.broadcast_to(m_sc[g], (AUG - TOP, WIDTH))


def attend(sides, qts, state, blocks, places, start=0, fresh=0, pooled=1, rows=()):
    count, groups = len(blocks), len(sides) * GROUPS
    before = rows[0].shape[0] if rows else 0
    rows_shape = (before + count, BEAC, 2 * HEAD)
    return pl.pallas_call(
        functools.partial(blocks_kernel, sides, start, fresh, pooled, before, places),
        out_shape=(
            jax.ShapeDtypeStruct((groups, AUG, WIDTH), F32),
            *[jax.ShapeDtypeStruct(rows_shape, BF16)] * pooled,
        ),
        in_specs=[
            *[QT_SPEC] * len(sides),
            whole(*state.shape),
            *[whole(ROWS, 2 * HEAD)] * count,
            *[whole(*r.shape) for r in rows],
        ],
        out_specs=(whole(groups, AUG, WIDTH), *[whole(*rows_shape)] * pooled),
        scratch_shapes=[
            pltpu.VMEM((groups, HEAD, WIDTH), BF16),
            pltpu.VMEM((groups, 1, WIDTH), F32),
            pltpu.VMEM((count, TOK, HEAD), BF16),
            pltpu.VMEM((count, AUG, TOK), BF16),
            pltpu.VMEM((TOK, WIDTH), F32),
            pltpu.VMEM((TOK, WIDTH), BF16),
            pltpu.VMEM((1, WIDTH), F32),
            pltpu.VMEM((1, WIDTH), F32),
            pltpu.SMEM((count * groups + 1,), jnp.int32),
        ],
        cost_estimate=cost(count * len(sides)),
        compiler_params=PARAMS,
        name="attend",
    )(*qts, state, *blocks, *rows)


def final_kernel(counts, places, q_ref, qt_ref, local_ref, mine_ref, sent_ref, *refs):
    beacon_refs = refs[: len(counts)]
    gap_hbm, grads_ref, gap_ref, kb_sc, vb_sc, vt_sc, s_sc, p_sc, grad_sc, gap_sc, sem = refs[len(counts) :]
    me = lax.axis_index("seq")
    kb_sc[...] = jnp.zeros_like(kb_sc)
    vb_sc[...] = jnp.zeros_like(vb_sc)
    n = 0
    for ref, count in zip(beacon_refs, counts):
        for i in range(count):
            at = pl.multiple_of(placed(me, *places[n]) * BEAC, BEAC)
            kb_sc[pl.ds(at, BEAC), :] = ref[i, :, 0:HEAD]
            vb_sc[pl.ds(at, BEAC), :] = ref[i, :, HEAD:]
            n += 1
    kb = kb_sc[...]
    vb = vb_sc[...]
    vt_sc[0:HEAD, :] = vb.T
    vt_sc[HEAD:, :] = jnp.ones((AUG - HEAD, SEQ * BEAC), BF16)
    seen = lax.broadcasted_iota(jnp.int32, (SEQ * BEAC, TOK), 0) < me * BEAC
    tops = []
    for h in range(HEADS):
        g, at = located(h)
        s = jnp.where(seen, dot(kb, qt_ref[g, :, at]), -1e30)
        s_sc[h] = s
        old = local_ref[g, TOP : TOP + 1, at]
        tops.append(jnp.maximum(old, jnp.max(s, axis=0, keepdims=True) * C2))
    for h in range(HEADS):
        p_sc[h] = jnp.exp2(s_sc[h] * C2 - tops[h]).astype(BF16)
    scaled = []
    for h in range(HEADS):
        g, at = located(h)
        old = jnp.exp2(local_ref[g, TOP : TOP + 1, at] - tops[h])
        student = local_ref[g, :, at] * old + dot(vt_sc[...], p_sc[h])
        inverse = 1.0 / student[SUM : SUM + 1, :]
        student = student[0:HEAD, :] * inverse
        old, new = mine_ref[g, TOP : TOP + 1, at], sent_ref[g, TOP : TOP + 1, at]
        top = jnp.maximum(old, new)
        old, new = jnp.exp2(old - top), jnp.exp2(new - top)
        total = mine_ref[g, SUM : SUM + 1, at] * old + sent_ref[g, SUM : SUM + 1, at] * new
        total = 1.0 / total
        teacher = mine_ref[g, 0:HEAD, at] * (old * total) + sent_ref[g, 0:HEAD, at] * (new * total)
        gap_t = (student - teacher).astype(BF16)
        gap_ref[:, span(h, HEAD)] = gap_t.T
        gap_t = gap_t.astype(F32) * inverse
        row_dot = jnp.sum(gap_t * student, axis=0, keepdims=True)
        gap_t = gap_t.astype(BF16)
        gap_sc[h] = gap_t.T
        scaled.append((gap_t, row_dot))
    gap_copy = pltpu.make_async_copy(gap_ref, gap_hbm, sem)
    gap_copy.start()
    for h in range(HEADS):
        gap_t, row_dot = scaled[h]
        grad_sc[h] = (p_sc[h].astype(F32) * (dot(vb, gap_t) - row_dot)).astype(BF16)
    grad_keys = dot(grad_sc[0], q_ref[:, span(0, HEAD)])
    grad_values = dot(p_sc[0], gap_sc[0])
    for h in range(1, HEADS):
        grad_keys = grad_keys + dot(grad_sc[h], q_ref[:, span(h, HEAD)])
        grad_values = grad_values + dot(p_sc[h], gap_sc[h])
    grads_ref[:, 0:HEAD] = (grad_keys * SCALE).astype(BF16)
    grads_ref[:, HEAD:] = grad_values.astype(BF16)
    gap_copy.wait()


def finish(queries, qt, states, beacons, places):
    counts = [b.shape[0] for b in beacons]
    return pl.pallas_call(
        functools.partial(final_kernel, counts, places),
        out_shape=(
            jax.ShapeDtypeStruct((TOK, HEADS * HEAD), BF16),
            pltpu.VMEM((SEQ * BEAC, 2 * HEAD), BF16),
        ),
        in_specs=[
            whole(TOK, HEADS * HEAD),
            QT_SPEC,
            *[STATE_SPEC] * len(states),
            *[whole(*b.shape) for b in beacons],
        ],
        out_specs=(pl.BlockSpec(memory_space=pl.ANY), whole(SEQ * BEAC, 2 * HEAD)),
        scratch_shapes=[
            pltpu.VMEM((TOK, HEADS * HEAD), BF16),
            pltpu.VMEM((SEQ * BEAC, HEAD), BF16),
            pltpu.VMEM((SEQ * BEAC, HEAD), BF16),
            pltpu.VMEM((AUG, SEQ * BEAC), BF16),
            pltpu.VMEM((HEADS, SEQ * BEAC, TOK), F32),
            pltpu.VMEM((HEADS, SEQ * BEAC, TOK), BF16),
            pltpu.VMEM((HEADS, SEQ * BEAC, TOK), BF16),
            pltpu.VMEM((HEADS, TOK, HEAD), BF16),
            pltpu.SemaphoreType.DMA,
        ],
        cost_estimate=cost(2),
        compiler_params=PARAMS,
        name="finish",
    )(queries, qt, *states, *beacons)


def moved(block, dx, dy, dc):
    return lax.ppermute(block, "seq", [(s, placed(s, dx, dy, dc)) for s in range(SEQ)])


def swapped(block):
    return moved(block, 0, 0, 1)


def layer(queries, teacher_keys, teacher_values, beacon_starts):
    own = prep(beacon_starts, teacher_keys, teacher_values)
    left = moved(own, 1, 0, 0)
    across = moved(own, 0, 1, 0)
    right = moved(own, 3, 0, 0)
    qt, state_local = local(queries, teacher_keys, teacher_values)
    qt_twin = swapped(qt)
    opposite = moved(own, 2, 1, 0)
    left2 = moved(left, 1, 0, 0)
    left_across = moved(left, 0, 1, 0)
    right_across = moved(across, 3, 0, 0)
    near = [own, left, across, right]
    near_places = [(0, 0, 0), (3, 0, 0), (0, 1, 0), (1, 0, 0)]
    middle_places = [(2, 1, 0)]
    far = [left2, left_across, right_across]
    far_places = [(2, 0, 0), (3, 1, 0), (1, 1, 0)]
    state, rows = attend(
        (0, 1), (qt, qt_twin), state_local, near, near_places, fresh=GROUPS
    )
    state, rows = attend(
        (0, 1), (qt, qt_twin), state, [opposite], middle_places, rows=(rows,)
    )
    lent, rows = attend(
        (1,), (qt_twin,), state, far, far_places, start=GROUPS, rows=(rows,)
    )
    sent = swapped(lent)
    twin_rows = swapped(rows)
    (mine,) = attend((0,), (qt,), state, far, far_places, pooled=0)
    places = near_places + middle_places + far_places
    places = places + [(dx, dy, 1) for dx, dy, _ in places]
    gap, grads = finish(queries, qt, (state_local, mine, sent), (rows, twin_rows), places)
    arrived = lax.all_to_all(grads.reshape(SEQ, BEAC, 2 * HEAD), "seq", 0, 0, tiled=True)
    key_rows, value_rows = (
        jnp.sum(part.astype(F32), axis=0) for part in jnp.split(arrived, 2, axis=2)
    )
    return gap, key_rows, value_rows


def solution(mesh):
    spec = P(("doc", "seq"), None)
    return jax.shard_map(
        layer,
        mesh=mesh,
        in_specs=(spec, spec, spec, P(("doc", "seq"))),
        out_specs=(spec, spec, spec),
        check_vma=False,
    )
```

```python
import functools

import jax
import jax.numpy as jnp
from jax import lax
from jax.experimental import pallas as pl
from jax.experimental.pallas import tpu as pltpu
from jax.sharding import PartitionSpec as P


HEADS = 4
HEAD = 128
TOK = 512
BEAC = 32
SEQ = 16
ROWS = TOK + BEAC
SCALE = HEAD**-0.5
LOG2E = 1.4426950408889634
C2 = SCALE * LOG2E
F32 = jnp.float32
BF16 = jnp.bfloat16


def dot(a, b):
    return jnp.dot(a, b, preferred_element_type=F32)


def split_index(s):
    return s // 4, (s // 2) % 2, s % 2


def placed(s, dx, dy, dc):
    x, y, c = split_index(s)
    return ((x + dx) % 4) * 4 + (y + dy) % 2 * 2 + (c + dc) % 2


def whole(*shape):
    return pl.BlockSpec(shape, lambda: tuple(0 for _ in shape))


def prep_kernel(starts_ref, keys_ref, values_ref, packed_ref):
    packed_ref[0:TOK, 0:HEAD] = keys_ref[...]
    packed_ref[0:TOK, HEAD:] = values_ref[...]
    pos = lax.broadcasted_iota(jnp.int32, (1, TOK), 1)
    owner = jnp.full((1, TOK), -1, jnp.int32)
    for j in range(BEAC):
        owner = owner + (pos >= starts_ref[j]).astype(jnp.int32)
    rows = lax.broadcasted_iota(jnp.int32, (BEAC, TOK), 0)
    member = (rows == owner).astype(F32)
    counts = jnp.sum(member, axis=1, keepdims=True)
    member = member.astype(BF16)
    packed_ref[TOK:, 0:HEAD] = (dot(member, keys_ref[...]) / counts).astype(BF16)
    packed_ref[TOK:, HEAD:] = (dot(member, values_ref[...]) / counts).astype(BF16)


def prep(starts, keys, values):
    return pl.pallas_call(
        prep_kernel,
        out_shape=pltpu.VMEM((ROWS, 2 * HEAD), BF16),
        in_specs=[
            pl.BlockSpec(memory_space=pltpu.SMEM),
            whole(TOK, HEAD),
            whole(TOK, HEAD),
        ],
        out_specs=whole(ROWS, 2 * HEAD),
        name="prep",
    )(starts, keys, values)


WIDTH = 1024
GROUPS = HEADS * TOK // WIDTH
AUG = HEAD + 16
SUM = HEAD
TOP = HEAD + 8
PARAMS = pltpu.CompilerParams(vmem_limit_bytes=16 * 2**20)
STATE = jax.ShapeDtypeStruct((GROUPS, AUG, WIDTH), F32)
STATE_SPEC = whole(GROUPS, AUG, WIDTH)
QT_SHAPE = jax.ShapeDtypeStruct((GROUPS, HEAD, WIDTH), BF16)
QT_SPEC = whole(GROUPS, HEAD, WIDTH)
PART = 256


def span(i, width=PART):
    return slice(i * width, (i + 1) * width)


def located(h, part=None):
    if part is None:
        g, at = divmod(h * TOK, WIDTH)
        return g, slice(at, at + TOK)
    g, at = divmod(h * TOK + part * PART, WIDTH)
    return g, slice(at, at + PART)


def local_kernel(queries_ref, keys_ref, values_ref, qt_ref, state_ref, vt_sc):
    vt_sc[0:HEAD, :] = values_ref[...].T
    vt_sc[HEAD:, :] = jnp.ones((AUG - HEAD, TOK), BF16)
    causal = lax.broadcasted_iota(jnp.int32, (PART, PART), 0) <= lax.broadcasted_iota(
        jnp.int32, (PART, PART), 1
    )
    for h in range(HEADS):
        for part in range(TOK // PART):
            g, at = located(h, part)
            qt = queries_ref[span(part), span(h, HEAD)].T
            qt_ref[g, :, at] = qt
            s = dot(keys_ref[span(part), :], qt)
            s = jnp.where(causal, s, -1e30)
            top = jnp.max(s, axis=0, keepdims=True)
            if part:
                past = dot(keys_ref[0 : part * PART, :], qt)
                top = jnp.maximum(top, jnp.max(past, axis=0, keepdims=True))
            top = top * C2
            p = jnp.exp2(s * C2 - top).astype(BF16)
            acc = dot(vt_sc[:, span(part)], p)
            if part:
                p = jnp.exp2(past * C2 - top).astype(BF16)
                acc = acc + dot(vt_sc[:, 0 : part * PART], p)
            state_ref[g, 0:TOP, at] = acc[0:TOP]
            state_ref[g, TOP:, at] = jnp.broadcast_to(top, (AUG - TOP, PART))


def cost(blocks):
    n = HEADS * TOK * TOK * blocks
    return pl.CostEstimate(flops=n * 4 * HEAD, transcendentals=n, bytes_accessed=2**20)


def local(queries, keys, values):
    return pl.pallas_call(
        local_kernel,
        out_shape=(QT_SHAPE, STATE),
        in_specs=[whole(TOK, HEADS * HEAD), whole(TOK, HEAD), whole(TOK, HEAD)],
        out_specs=(QT_SPEC, STATE_SPEC),
        scratch_shapes=[pltpu.VMEM((AUG, TOK), BF16)],
        cost_estimate=cost(1),
        compiler_params=PARAMS,
        name="local",
    )(*[pltpu.with_memory_space_constraint(a, pltpu.HBM) for a in (queries, keys, values)])


def blocks_kernel(sides, start, fresh, pooled, before, places, *refs):
    count = len(places)
    groups = len(sides) * GROUPS
    me = lax.axis_index("seq")
    qt_refs, refs = refs[: len(sides)], refs[len(sides) :]
    in_ref, refs = refs[0], refs[1:]
    block_refs, refs = refs[:count], refs[count:]
    if before:
        before_ref, refs = refs[0], refs[1:]
    acc_ref, refs = refs[0], refs[1:]
    if pooled:
        beacons_ref, refs = refs[0], refs[1:]
    qt_sc, m_sc, k_sc, vt_sc, s_sc, p_sc, top_sc, alpha_sc, tile_ref = refs
    for g in range(groups):
        qt_sc[g] = qt_refs[g // GROUPS][g % GROUPS]
        if g < groups - fresh:
            acc_ref[g] = in_ref[start + g]
            m_sc[g] = in_ref[start + g, TOP : TOP + 1, :]
        else:
            acc_ref[g] = jnp.zeros((AUG, WIDTH), F32)
            m_sc[g] = jnp.full((1, WIDTH), -1e30, F32)
    tiles = jnp.int32(0)
    for i in range(count):
        for n, side in enumerate(sides):
            seen = (placed(me, *places[i]) < placed(me, 0, 0, side)).astype(jnp.int32)
            for g in range(GROUPS):
                tile_ref[tiles] = i * groups + n * GROUPS + g
                tiles = tiles + seen
        k_sc[i] = block_refs[i][0:TOK, 0:HEAD]

    def where_is(t):
        tile = tile_ref[t]
        return tile // groups, tile % groups

    def score(t):
        i, g = where_is(t)
        s = dot(k_sc[i], qt_sc[g])
        s_sc[...] = s
        top_sc[...] = jnp.max(s, axis=0, keepdims=True) * C2

    def weigh(t):
        _, g = where_is(t)
        old = m_sc[g]
        top = jnp.maximum(old, top_sc[...])
        m_sc[g] = top
        alpha_sc[...] = jnp.exp2(old - top)
        p_sc[...] = jnp.exp2(s_sc[...] * C2 - top).astype(BF16)

    def gather(t):
        i, g = where_is(t)
        acc_ref[g] = acc_ref[g] * alpha_sc[...] + dot(vt_sc[i], p_sc[...])

    def step(t, carry):
        gather(t - 1)
        weigh(t)
        score(t + 1)
        return carry

    score(0)
    for i in range(count):
        vt_sc[i, 0:HEAD, :] = block_refs[i][0:TOK, HEAD:].T
        vt_sc[i, HEAD:, :] = jnp.ones((AUG - HEAD, TOK), BF16)
        if pooled:
            beacons_ref[before + i] = block_refs[i][TOK:, :]
    if before:
        beacons_ref[0:before] = before_ref[...]

    @pl.when(tiles > 0)
    def _():
        weigh(0)
        score(1)
        lax.fori_loop(1, tiles - 1, step, 0)
        gather(tiles - 2)
        weigh(tiles - 1)
        gather(tiles - 1)

    for g in range(groups):
        acc_ref[g, TOP:] = jnp.broadcast_to(m_sc[g], (AUG - TOP, WIDTH))


def attend(sides, qts, state, blocks, places, start=0, fresh=0, pooled=1, rows=()):
    count, groups = len(blocks), len(sides) * GROUPS
    before = rows[0].shape[0] if rows else 0
    rows_shape = (before + count, BEAC, 2 * HEAD)
    return pl.pallas_call(
        functools.partial(blocks_kernel, sides, start, fresh, pooled, before, places),
        out_shape=(
            jax.ShapeDtypeStruct((groups, AUG, WIDTH), F32),
            *[jax.ShapeDtypeStruct(rows_shape, BF16)] * pooled,
        ),
        in_specs=[
            *[QT_SPEC] * len(sides),
            whole(*state.shape),
            *[whole(ROWS, 2 * HEAD)] * count,
            *[whole(*r.shape) for r in rows],
        ],
        out_specs=(whole(groups, AUG, WIDTH), *[whole(*rows_shape)] * pooled),
        scratch_shapes=[
            pltpu.VMEM((groups, HEAD, WIDTH), BF16),
            pltpu.VMEM((groups, 1, WIDTH), F32),
            pltpu.VMEM((count, TOK, HEAD), BF16),
            pltpu.VMEM((count, AUG, TOK), BF16),
            pltpu.VMEM((TOK, WIDTH), F32),
            pltpu.VMEM((TOK, WIDTH), BF16),
            pltpu.VMEM((1, WIDTH), F32),
            pltpu.VMEM((1, WIDTH), F32),
            pltpu.SMEM((count * groups + 1,), jnp.int32),
        ],
        cost_estimate=cost(count * len(sides)),
        compiler_params=PARAMS,
        name="attend",
    )(*qts, state, *blocks, *rows)


def final_kernel(counts, places, q_ref, qt_ref, local_ref, mine_ref, sent_ref, *refs):
    beacon_refs = refs[: len(counts)]
    gap_hbm, grads_ref, gap_ref, kb_sc, vb_sc, vt_sc, s_sc, p_sc, grad_sc, gap_sc, sem = refs[len(counts) :]
    me = lax.axis_index("seq")
    kb_sc[...] = jnp.zeros_like(kb_sc)
    vb_sc[...] = jnp.zeros_like(vb_sc)
    n = 0
    for ref, count in zip(beacon_refs, counts):
        for i in range(count):
            at = pl.multiple_of(placed(me, *places[n]) * BEAC, BEAC)
            kb_sc[pl.ds(at, BEAC), :] = ref[i, :, 0:HEAD]
            vb_sc[pl.ds(at, BEAC), :] = ref[i, :, HEAD:]
            n += 1
    kb = kb_sc[...]
    vb = vb_sc[...]
    vt_sc[0:HEAD, :] = vb.T
    vt_sc[HEAD:, :] = jnp.ones((AUG - HEAD, SEQ * BEAC), BF16)
    seen = lax.broadcasted_iota(jnp.int32, (SEQ * BEAC, TOK), 0) < me * BEAC
    tops = []
    for h in range(HEADS):
        g, at = located(h)
        s = jnp.where(seen, dot(kb, qt_ref[g, :, at]), -1e30)
        s_sc[h] = s
        old = local_ref[g, TOP : TOP + 1, at]
        tops.append(jnp.maximum(old, jnp.max(s, axis=0, keepdims=True) * C2))
    for h in range(HEADS):
        p_sc[h] = jnp.exp2(s_sc[h] * C2 - tops[h]).astype(BF16)
    scaled = []
    for h in range(HEADS):
        g, at = located(h)
        old = jnp.exp2(local_ref[g, TOP : TOP + 1, at] - tops[h])
        student = local_ref[g, :, at] * old + dot(vt_sc[...], p_sc[h])
        inverse = 1.0 / student[SUM : SUM + 1, :]
        student = student[0:HEAD, :] * inverse
        old, new = mine_ref[g, TOP : TOP + 1, at], sent_ref[g, TOP : TOP + 1, at]
        top = jnp.maximum(old, new)
        old, new = jnp.exp2(old - top), jnp.exp2(new - top)
        total = mine_ref[g, SUM : SUM + 1, at] * old + sent_ref[g, SUM : SUM + 1, at] * new
        total = 1.0 / total
        teacher = mine_ref[g, 0:HEAD, at] * (old * total) + sent_ref[g, 0:HEAD, at] * (new * total)
        gap_t = (student - teacher).astype(BF16)
        gap_ref[:, span(h, HEAD)] = gap_t.T
        gap_t = gap_t.astype(F32) * inverse
        row_dot = jnp.sum(gap_t * student, axis=0, keepdims=True)
        gap_t = gap_t.astype(BF16)
        gap_sc[h] = gap_t.T
        scaled.append((gap_t, row_dot))
    gap_copy = pltpu.make_async_copy(gap_ref, gap_hbm, sem)
    gap_copy.start()
    for h in range(HEADS):
        gap_t, row_dot = scaled[h]
        grad_sc[h] = (p_sc[h].astype(F32) * (dot(vb, gap_t) - row_dot)).astype(BF16)
    grad_keys = dot(grad_sc[0], q_ref[:, span(0, HEAD)])
    grad_values = dot(p_sc[0], gap_sc[0])
    for h in range(1, HEADS):
        grad_keys = grad_keys + dot(grad_sc[h], q_ref[:, span(h, HEAD)])
        grad_values = grad_values + dot(p_sc[h], gap_sc[h])
    grads_ref[:, 0:HEAD] = (grad_keys * SCALE).astype(BF16)
    grads_ref[:, HEAD:] = grad_values.astype(BF16)
    gap_copy.wait()


def finish(queries, qt, states, beacons, places):
    counts = [b.shape[0] for b in beacons]
    return pl.pallas_call(
        functools.partial(final_kernel, counts, places),
        out_shape=(
            jax.ShapeDtypeStruct((TOK, HEADS * HEAD), BF16),
            pltpu.VMEM((SEQ * BEAC, 2 * HEAD), BF16),
        ),
        in_specs=[
            whole(TOK, HEADS * HEAD),
            QT_SPEC,
            *[STATE_SPEC] * len(states),
            *[whole(*b.shape) for b in beacons],
        ],
        out_specs=(pl.BlockSpec(memory_space=pl.ANY), whole(SEQ * BEAC, 2 * HEAD)),
        scratch_shapes=[
            pltpu.VMEM((TOK, HEADS * HEAD), BF16),
            pltpu.VMEM((SEQ * BEAC, HEAD), BF16),
            pltpu.VMEM((SEQ * BEAC, HEAD), BF16),
            pltpu.VMEM((AUG, SEQ * BEAC), BF16),
            pltpu.VMEM((HEADS, SEQ * BEAC, TOK), F32),
            pltpu.VMEM((HEADS, SEQ * BEAC, TOK), BF16),
            pltpu.VMEM((HEADS, SEQ * BEAC, TOK), BF16),
            pltpu.VMEM((HEADS, TOK, HEAD), BF16),
            pltpu.SemaphoreType.DMA,
        ],
        cost_estimate=cost(2),
        compiler_params=PARAMS,
        name="finish",
    )(queries, qt, *states, *beacons)


def moved(block, dx, dy, dc):
    return lax.ppermute(block, "seq", [(s, placed(s, dx, dy, dc)) for s in range(SEQ)])


def swapped(block):
    return moved(block, 0, 0, 1)


def layer(queries, teacher_keys, teacher_values, beacon_starts):
    own = prep(beacon_starts, teacher_keys, teacher_values)
    left = moved(own, 1, 0, 0)
    across = moved(own, 0, 1, 0)
    right = moved(own, 3, 0, 0)
    qt, state_local = local(queries, teacher_keys, teacher_values)
    qt_twin = swapped(qt)
    opposite = moved(own, 2, 1, 0)
    left2 = moved(left, 1, 0, 0)
    left_across = moved(left, 0, 1, 0)
    right_across = moved(across, 3, 0, 0)
    near = [own, left, across, right]
    near_places = [(0, 0, 0), (3, 0, 0), (0, 1, 0), (1, 0, 0)]
    middle_places = [(2, 1, 0)]
    far = [left2, left_across, right_across]
    far_places = [(2, 0, 0), (3, 1, 0), (1, 1, 0)]
    state, rows = attend(
        (0, 1), (qt, qt_twin), state_local, near, near_places, fresh=GROUPS
    )
    state, rows = attend(
        (0, 1), (qt, qt_twin), state, [opposite], middle_places, rows=(rows,)
    )
    lent, rows = attend(
        (1,), (qt_twin,), state, far, far_places, start=GROUPS, rows=(rows,)
    )
    sent = swapped(lent)
    twin_rows = swapped(rows)
    (mine,) = attend((0,), (qt,), state, far, far_places, pooled=0)
    places = near_places + middle_places + far_places
    places = places + [(dx, dy, 1) for dx, dy, _ in places]
    gap, grads = finish(queries, qt, (state_local, mine, sent), (rows, twin_rows), places)
    arrived = lax.all_to_all(grads.reshape(SEQ, BEAC, 2 * HEAD), "seq", 0, 0, tiled=True)
    key_rows, value_rows = (
        jnp.sum(part.astype(F32), axis=0) for part in jnp.split(arrived, 2, axis=2)
    )
    return gap, key_rows, value_rows


def solution(mesh):
    spec = P(("doc", "seq"), None)
    return jax.shard_map(
        layer,
        mesh=mesh,
        in_specs=(spec, spec, spec, P(("doc", "seq"))),
        out_specs=(spec, spec, spec),
        check_vma=False,
    )
```
